256 devices in a mesh: row: 32 (over x, z_lo, core), col: 8 (over y, z_hi).
Axes of the slice: x: 4, y: 4, z: 8 (z_hi: 2, z_lo: 4; z = z_hi * 4 + z_lo), core: 2. Of those that a mesh axis runs over, the one named last changes fastest.
Arguments:
- node_states: bfloat16 [131072, 256], P(('row', 'col')), may hold values from -6 to 6
- neighbours: int32 [131072, 16], P(('row', 'col')), may hold values from 0 to 131071, as said below
- counts: int32 [131072], P(('row', 'col')), may hold values from 1 to 16
- virtual_states: bfloat16 [64, 256], replicated, may hold values from -6 to 6
- norm_gain: float32 [256], replicated, may hold values from 0.25 to 1.75
- qkv_weight: bfloat16 [256, 768], replicated, may hold values from -3 to 3
- out_weight: bfloat16 [256, 256], replicated, may hold values from -0.375 to 0.375
Outputs:
- node_out: bfloat16 [131072, 256], P(('row', 'col'))
- virtual_out: bfloat16 [64, 256], replicated
The draws below stay inside these ranges and needn't reach their ends.
Inputs may be any that keep to these rules, and one draw needn't show every extreme that they name: `neighbours`: every neighbour id, live or dead, names a node on a device with the same row index or the same col index as the device of node n, with the device of n numbered n // 512 and its row index = that number // 8. All slots of the nodes of one device name at most 128 distinct nodes of any one device (its own included), and on every device the live slots name exactly 128 distinct nodes of some one device.
All inputs are finite; a program needn't handle non-finite values.
Results may differ from the reference program's by a relative error of at most 0.001.
The reference program's roundings to bfloat16 on the way count: a program that leaves them out, or rounds other values in their place, can miss the bound.
Values may be sent and summed in bfloat16 or wider, within the bound.
No kernel may reach another device: no remote copies, remote signals or barrier semaphores. Data moves between devices by JAX's collectives and lax.ppermute only.
A program may use at most 128 MiB of HBM per device.

```python
import jax
import jax.numpy as jnp
from jax import lax

D = 256
HEADS = 8
HEAD_DIM = 32
DEG = 16
VIRT = 64
NODE_DEV = 512
TOUCH = 128
NODES = 131072
N_ROW = 32
N_COL = 8


def live_counts(key):
    return jax.random.randint(jax.random.fold_in(key, 61), (NODES,), 1, DEG + 1).astype(jnp.int32)


def neighbour_ids(key):
    devices = N_ROW * N_COL
    node_ids = jnp.arange(NODE_DEV * devices, dtype=jnp.int32)
    device = node_ids // NODE_DEV
    local_node = node_ids % NODE_DEV
    grid_row = device // N_COL
    grid_col = device % N_COL
    shape = (NODE_DEV * devices, DEG)
    side = jax.random.randint(jax.random.fold_in(key, 11), shape, 0, 2)
    other_col = jax.random.randint(jax.random.fold_in(key, 12), shape, 0, N_COL)
    other_row = (grid_row[:, None] + 1 + jax.random.randint(jax.random.fold_in(key, 13), shape, 0, N_ROW - 1)) % N_ROW
    pick = jax.random.randint(jax.random.fold_in(key, 14), shape, 0, TOUCH)
    limit = (2 ** 31 - 1) // NODE_DEV
    ranking = jax.random.randint(jax.random.fold_in(key, 15), (devices, N_COL + N_ROW, NODE_DEV), 0, limit) * NODE_DEV + jnp.arange(NODE_DEV, dtype=jnp.int32)[None, None, :]
    touched = jnp.argsort(ranking, axis=-1)[:, :, :TOUCH].astype(jnp.int32)
    star = jax.random.randint(jax.random.fold_in(key, 16), (devices,), 0, N_COL)
    first = (jnp.arange(DEG, dtype=jnp.int32)[None, :] == 0) & (local_node[:, None] < TOUCH)
    side = jnp.where(first, 0, side)
    other_col = jnp.where(first, star[device][:, None], other_col)
    pick = jnp.where(first, local_node[:, None], pick)
    table = jnp.where(side == 0, other_col, N_COL + other_row)
    local_ids = touched[device[:, None], table, pick]
    same_row = (grid_row[:, None] * N_COL + other_col) * NODE_DEV + local_ids
    same_col = (other_row * N_COL + grid_col[:, None]) * NODE_DEV + local_ids
    return jnp.where(side == 0, same_row, same_col).astype(jnp.int32)


def draw_neighbours(key, part):
    return neighbour_ids(key)


def draw_counts(key, part):
    return live_counts(key)


def draw_node_states(key, part):
    states = jax.random.normal(jax.random.fold_in(key, 21), (NODES, D), jnp.float32)
    return jnp.clip(states, -6.0, 6.0).astype(jnp.bfloat16)


def draw_virtual_states(key, part):
    states = jax.random.normal(jax.random.fold_in(key, 31), (VIRT, D), jnp.float32)
    return jnp.clip(states, -6.0, 6.0).astype(jnp.bfloat16)


def draw_qkv_weight(key, part):
    spread = jnp.float32(D) ** (-0.5)
    weight = jnp.clip(jax.random.normal(jax.random.fold_in(key, 41), (D, 3 * D), jnp.float32), -6.0, 6.0) * spread
    return jnp.clip(weight, -3.0, 3.0).astype(jnp.bfloat16)


def gaussian(rng, dims, scale, most, kind=jnp.bfloat16):
    return jnp.clip(scale * jax.random.normal(rng, dims, jnp.float32), -most, most).astype(kind)


def setup_inputs(seed: int = 0) -> dict:
    key_list = jax.random.split(jax.random.key(seed), 8)
    return {
        "node_states": draw_node_states(jax.random.fold_in(key_list[7], 71), 0),
        "neighbours": draw_neighbours(jax.random.fold_in(key_list[7], 71), 0),
        "counts": draw_counts(jax.random.fold_in(key_list[7], 71), 0),
        "virtual_states": draw_virtual_states(jax.random.fold_in(key_list[7], 71), 0),
        "norm_gain": jnp.clip(1.0 + 0.15 * jax.random.normal(key_list[4], (D,), jnp.float32), 0.25, 1.75),
        "qkv_weight": draw_qkv_weight(jax.random.fold_in(key_list[7], 71), 0),
        "out_weight": gaussian(key_list[6], (D, D), D ** -0.5, 0.375),
    }


def normed_rows(states, norm_gain):
    wide = states.astype(jnp.float32)
    factor = lax.rsqrt(lax.optimization_barrier(jnp.mean(wide * wide, axis=-1, keepdims=True)) + 1e-05)
    return (wide * factor * norm_gain).astype(jnp.bfloat16)

def project_all(states, norm_gain, qkv_weight):
    hidden = normed_rows(states, norm_gain)
    joined = jnp.dot(hidden, qkv_weight, preferred_element_type=jnp.float32).astype(jnp.bfloat16)
    return (joined[:, :D], joined[:, D:2 * D], joined[:, 2 * D:])

def reference(node_states, neighbours, counts, virtual_states, norm_gain, qkv_weight, out_weight):
    highest = lax.Precision.HIGHEST
    score_scale = HEAD_DIM ** (-0.5)
    queries, keys_all, values_all = project_all(node_states, norm_gain, qkv_weight)
    virt_q, virt_k, virt_v = project_all(virtual_states, norm_gain, qkv_weight)
    virt_kf = virt_k.astype(jnp.float32).reshape(VIRT, HEADS, HEAD_DIM)
    virt_vf = virt_v.astype(jnp.float32).reshape(VIRT, HEADS, HEAD_DIM)
    blocks = NODES // NODE_DEV

    def node_block(inputs):
        query_block, neighbour_block, count_block = inputs
        rows = query_block.shape[0]
        query_heads = query_block.astype(jnp.float32).reshape(rows, HEADS, HEAD_DIM)
        near_keys = keys_all[neighbour_block].astype(jnp.float32).reshape(rows, DEG, HEADS, HEAD_DIM)
        near_values = values_all[neighbour_block].astype(jnp.float32).reshape(rows, DEG, HEADS, HEAD_DIM)
        near_scores = jnp.einsum('bhd,bjhd->bhj', query_heads, near_keys, precision=highest) * score_scale
        live_slot = jnp.arange(DEG)[None, None, :] < count_block[:, None, None]
        near_scores = jnp.where(live_slot, near_scores, -1e+30)
        virt_scores = jnp.einsum('bhd,uhd->bhu', query_heads, virt_kf, precision=highest) * score_scale
        weights = jax.nn.softmax(jnp.concatenate([near_scores, virt_scores], axis=-1), axis=-1)
        context = jnp.einsum('bhj,bjhd->bhd', weights[..., :DEG], near_values, precision=highest)
        context = context + jnp.einsum('bhu,uhd->bhd', weights[..., DEG:], virt_vf, precision=highest)
        return context.reshape(rows, D).astype(jnp.bfloat16)
    context = lax.map(node_block, (queries.reshape(blocks, NODE_DEV, D), neighbours.reshape(blocks, NODE_DEV, DEG), counts.reshape(blocks, NODE_DEV)))
    context = context.reshape(NODES, D)
    node_out = (node_states.astype(jnp.float32) + jnp.dot(context, out_weight, preferred_element_type=jnp.float32)).astype(jnp.bfloat16)
    virt_qh = virt_q.astype(jnp.float32).reshape(VIRT, HEADS, HEAD_DIM)
    keys_f = keys_all.astype(jnp.float32).reshape(NODES, HEADS, HEAD_DIM)
    values_f = values_all.astype(jnp.float32).reshape(NODES, HEADS, HEAD_DIM)
    far_scores = jnp.einsum('uhd,nhd->uhn', virt_qh, keys_f, precision=highest) * score_scale
    own_scores = jnp.einsum('uhd,whd->uhw', virt_qh, virt_kf, precision=highest) * score_scale
    weights = jax.nn.softmax(jnp.concatenate([far_scores, own_scores], axis=-1), axis=-1)
    virt_context = jnp.einsum('uhn,nhd->uhd', weights[..., :NODES], values_f, precision=highest)
    virt_context = virt_context + jnp.einsum('uhw,whd->uhd', weights[..., NODES:], virt_vf, precision=highest)
    virt_context = virt_context.reshape(VIRT, D).astype(jnp.bfloat16)
    virtual_out = (virtual_states.astype(jnp.float32) + jnp.dot(virt_context, out_weight, preferred_element_type=jnp.float32)).astype(jnp.bfloat16)
    return (node_out, virtual_out)
```

```python
import jax
import jax.numpy as jnp
from jax import lax
from jax.experimental import pallas as pl
from jax.experimental.pallas import tpu as pltpu
from jax.sharding import Mesh
from jax.sharding import PartitionSpec as P

D = 256
HEADS = 8
HEAD_DIM = 32
DEG = 16
VIRT = 64
ROWS = 512
BLOCK = 64
STEPS = ROWS // BLOCK
TABLE = 39
AXES = ("row_0", "row_1", "row_2", "col_0", "col_1")
SIZES = {"row_0": 4, "row_1": 4, "row_2": 2, "col_0": 4, "col_1": 2}
SCALE = HEAD_DIM ** (-0.5)
F32 = jnp.float32
BF16 = jnp.bfloat16


def shift(value, axis, step):
    n = SIZES[axis]
    return lax.ppermute(value, axis, [(i, (i + step) % n) for i in range(n)])


def dot(a, b, dims=(((1,), (0,)), ((), ()))):
    return lax.dot_general(a, b, dims, preferred_element_type=F32)


def halves(a):
    high = a.astype(BF16)
    return high, (a - high.astype(F32)).astype(BF16)


def normed(wide, gain):
    factor = lax.rsqrt(jnp.mean(wide * wide, axis=-1, keepdims=True) + 1e-05)
    return (wide * factor * gain).astype(BF16)


def head_of_lane(rows):
    return lax.broadcasted_iota(jnp.int32, (rows, D), 1) // HEAD_DIM


def by_head(a):
    wide = a.astype(F32)
    lane = head_of_lane(a.shape[0])
    return jnp.concatenate(
        [jnp.where(lane == h, wide, 0.0).astype(BF16) for h in range(HEADS)], axis=0
    )


def far_part(queries_bd, keys, values):
    scores = dot(queries_bd, keys, (((1,), (1,)), ((), ()))) * SCALE
    best = jnp.max(scores, axis=-1, keepdims=True)
    weights = jnp.exp(scores - best)
    total = jnp.sum(weights, axis=-1, keepdims=True)
    high, low = halves(weights)
    summed = dot(high, values) + dot(low, values)
    lane = head_of_lane(VIRT)
    small = lax.broadcasted_iota(jnp.int32, (VIRT, 128), 1)
    acc = jnp.zeros((VIRT, D), F32)
    stat = jnp.zeros((VIRT, 128), F32)
    for h in range(HEADS):
        at = slice(h * VIRT, (h + 1) * VIRT)
        acc = jnp.where(lane == h, summed[at], acc)
        stat = jnp.where(small == h, best[at], stat)
        stat = jnp.where(small == HEADS + h, total[at], stat)
    return acc, stat


def local_kernel(x_ref, virt_ref, gain_ref, w_ref, q_ref, m_ref, l_ref, a_ref, part_ref, own_ref):
    gain = gain_ref[...]
    w = w_ref[...]
    hidden = normed(x_ref[...].astype(F32), gain)
    joined = dot(hidden, w).astype(BF16)
    queries, keys, values = joined[:, :D], joined[:, D : 2 * D], joined[:, 2 * D :]
    virt_joined = dot(normed(virt_ref[...].astype(F32), gain), w).astype(BF16)
    vq, vk, vv = virt_joined[:, :D], virt_joined[:, D : 2 * D], virt_joined[:, 2 * D :]
    q_ref[...] = queries
    vq_bd = by_head(vq)
    acc, stat = far_part(vq_bd, keys, values)
    part_ref[:, :D] = acc
    part_ref[:, D:] = stat
    acc, stat = far_part(vq_bd, vk, vv)
    own_ref[:, :D] = acc
    own_ref[:, D:] = stat
    scores = dot(by_head(vk), queries, (((1,), (1,)), ((), ()))) * SCALE
    scores = scores.reshape(HEADS, VIRT, ROWS)
    best = jnp.max(scores, axis=1, keepdims=True)
    weights = jnp.exp(scores - best)
    total = jnp.sum(weights, axis=1, keepdims=True)
    high, low = halves(weights.reshape(HEADS * VIRT, ROWS))
    vv_bd = by_head(vv)
    turn = (((0,), (0,)), ((), ()))
    summed = dot(vv_bd, high, turn) + dot(vv_bd, low, turn)
    a_ref[...] = summed.T
    m_ref[...] = jnp.broadcast_to(best, (HEADS, HEAD_DIM, ROWS)).reshape(D, ROWS).T
    l_ref[...] = jnp.broadcast_to(total, (HEADS, HEAD_DIM, ROWS)).reshape(D, ROWS).T


def spread(stat, first):
    lane = head_of_lane(VIRT)
    out = jnp.zeros((VIRT, D), F32)
    for h in range(HEADS):
        out = jnp.where(lane == h, stat[:, first + h : first + h + 1], out)
    return out


def merge(a, b):
    a_stat, b_stat = a[:, D:], b[:, D:]
    lane = lax.broadcasted_iota(jnp.int32, (VIRT, 128), 1)
    best = jnp.maximum(a_stat, b_stat)
    top = lane < HEADS
    a_scale = jnp.where(top, jnp.exp(jnp.where(top, a_stat - best, 0.0)), 0.0)
    b_scale = jnp.where(top, jnp.exp(jnp.where(top, b_stat - best, 0.0)), 0.0)
    total = a_stat * pltpu.roll(a_scale, HEADS, 1) + b_stat * pltpu.roll(b_scale, HEADS, 1)
    stat = jnp.where(top, best, total)
    acc = a[:, :D] * spread(a_scale, 0) + b[:, :D] * spread(b_scale, 0)
    return acc, stat


def merge_kernel(first_ref, mine_ref, other_ref, out_ref):
    mine, other = mine_ref[...], other_ref[...]
    first = first_ref[0] == 1
    acc, stat = merge(jnp.where(first, mine, other), jnp.where(first, other, mine))
    out_ref[:, :D] = acc
    out_ref[:, D:] = stat


def virtual_kernel(part_ref, own_ref, virt_ref, wo_ref, out_ref):
    acc, stat = merge(part_ref[...], own_ref[...])
    context = (acc / spread(stat, HEADS)).astype(BF16)
    out_ref[...] = (virt_ref[...].astype(F32) + dot(context, wo_ref[...])).astype(BF16)


def node_kernel(n_in, *refs):
    idx_ref, x_ref, q_ref, m_ref, l_ref, a_ref, cnt_ref, gain_ref, wkv_ref, wo_ref = refs[:10]
    blocks = refs[10 : 10 + n_in]
    out_ref, stage, table, rows, sems = refs[10 + n_in :]
    copies, at = [], 0
    for b in blocks:
        for k in range(b.shape[0] // ROWS):
            c = pltpu.make_async_copy(
                b.at[pl.ds(k * ROWS, ROWS)], stage.at[pl.ds(at * ROWS, ROWS)], sems.at[at]
            )
            c.start()
            copies.append(c)
            at += 1
    for t in range(TABLE):
        copies[t].wait()

        def widen(i, _):
            r = pl.multiple_of(t * ROWS + i * 64, 64)
            piece = stage[pl.ds(r, 64), :].astype(F32)
            table[0, pl.ds(r, 64), :] = piece[:, :128]
            table[1, pl.ds(r, 64), :] = piece[:, 128:]
            return 0

        lax.fori_loop(0, ROWS // 64, widen, 0)

    def gather(i, _):
        base = pl.multiple_of(i * 16, 16)
        for u in range(16):
            r = idx_ref[base + u]
            rows[0, pl.ds(base + u, 1), :] = table[0, pl.ds(r, 1), :]
            rows[1, pl.ds(base + u, 1), :] = table[1, pl.ds(r, 1), :]
        return 0

    lax.fori_loop(0, ROWS * DEG // 16, gather, 0)
    gain = gain_ref[...]
    lane = lax.broadcasted_iota(jnp.int32, (D, D), 0) // HEAD_DIM
    across = lax.broadcasted_iota(jnp.int32, (D, D), 1) // HEAD_DIM
    same = jnp.where(lane == across, 1.0, 0.0).astype(BF16)

    def attend(i, _):
        base = pl.multiple_of(i * BLOCK * DEG, BLOCK * DEG)
        n0 = pl.multiple_of(i * BLOCK, BLOCK)
        here = pl.ds(n0, BLOCK)
        x0 = rows[0, pl.ds(base, BLOCK * DEG), :]
        x1 = rows[1, pl.ds(base, BLOCK * DEG), :]
        mean = jnp.sum(x0 * x0 + x1 * x1, axis=-1, keepdims=True) * (1.0 / D)
        factor = lax.rsqrt(mean + 1e-05)
        hidden = jnp.concatenate(
            [
                (x0 * factor * gain[:, :128]).astype(BF16),
                (x1 * factor * gain[:, 128:]).astype(BF16),
            ],
            axis=1,
        )
        joined = dot(hidden, wkv_ref[...]).astype(BF16).astype(F32)
        query = q_ref[here, :].astype(F32)
        product = joined[:, :D].reshape(DEG, BLOCK, D) * query[None]
        high, low = halves(product.reshape(DEG * BLOCK, D))
        scores = (dot(high, same) + dot(low, same)) * SCALE
        scores = scores.reshape(DEG, BLOCK, D)
        slot = lax.broadcasted_iota(jnp.int32, (DEG, BLOCK, D), 0)
        scores = jnp.where(slot < cnt_ref[here, :][None], scores, -1e30)
        old = m_ref[here, :]
        best = jnp.maximum(old, jnp.max(scores, axis=0))
        weights = jnp.exp(scores - best[None])
        keep = jnp.exp(old - best)
        total = l_ref[here, :] * keep + jnp.sum(weights, axis=0)
        summed = a_ref[here, :] * keep + jnp.sum(
            weights * joined[:, D:].reshape(DEG, BLOCK, D), axis=0
        )
        context = (summed / total).astype(BF16)
        out_ref[here, :] = (x_ref[here, :].astype(F32) + dot(context, wo_ref[...])).astype(BF16)
        return 0

    lax.fori_loop(0, STEPS, attend, 0)


def vmem(n):
    return [pl.BlockSpec(memory_space=pltpu.VMEM)] * n


def cost(flops, moved):
    return pl.CostEstimate(flops=flops, bytes_accessed=moved, transcendentals=0)


def table_rows(neighbours):
    x, z, c = lax.axis_index("row_0"), lax.axis_index("row_1"), lax.axis_index("row_2")
    y, w = lax.axis_index("col_0"), lax.axis_index("col_1")
    device, local = neighbours // ROWS, neighbours % ROWS
    nw, ny, nc = device % 2, device // 2 % 4, device // 8 % 2
    nz, nx = device // 16 % 4, device // 64
    dx, dz, dy = (x - nx) % 4, (z - nz) % 4, (y - ny) % 4
    dw = jnp.where(nw == w, 0, 1)
    along_row = jnp.where(dx == 1, 4, jnp.where(dx == 3, 8, jnp.where(dx == 2, 12, 0)))
    along_row = along_row + dz + jnp.where(nc == c, 0, 16)
    along_col = jnp.where(dy == 0, 32 * dw, 31 + dw + 2 * jnp.where(dy == 1, 1, jnp.where(dy == 3, 2, 3)))
    mine = (nx == x) & (nz == z) & (nc == c)
    return jnp.where(mine, along_col, along_row) * ROWS + local


def reduce_virtual(part):
    pairs = {
        "near": [(0, 1), (1, 0), (2, 3), (3, 2)],
        "ring": [(1, 2), (2, 1), (0, 3), (3, 0)],
        "two": [(0, 2), (2, 0), (1, 3), (3, 1)],
        "both": [(0, 1), (1, 0)],
    }
    stages = (
        ("row_2", "both", 1),
        ("row_0", "near", 1),
        ("row_0", "ring", 2),
        ("col_0", "near", 1),
        ("col_0", "ring", 2),
        ("row_1", "near", 1),
        ("row_1", "two", 2),
        ("col_1", "both", 1),
    )
    for axis, kind, group in stages:
        other = lax.ppermute(part, axis, pairs[kind])
        first = (lax.axis_index(axis) // group % 2 == 0).astype(jnp.int32).reshape(1)
        part = pl.pallas_call(
            merge_kernel,
            out_shape=jax.ShapeDtypeStruct(part.shape, F32),
            in_specs=[pl.BlockSpec(memory_space=pltpu.SMEM)] + vmem(2),
            out_specs=pl.BlockSpec(memory_space=pltpu.VMEM),
            cost_estimate=cost(2_000_000, 300_000),
            name="merge",
        )(first, part, other)
    return part


def shards(node_states, neighbours, counts, virtual_states, norm_gain, qkv_weight, out_weight):
    gain = norm_gain.reshape(1, D)
    own = node_states
    w_block = shift(own, "col_1", 1)
    z1, z2, z3 = (shift(own, "row_1", k) for k in (1, 2, 3))
    ga = jnp.concatenate([own, z1], axis=0)
    gb = jnp.concatenate([z2, z3], axis=0)
    xpa, xma = shift(ga, "row_0", 1), shift(ga, "row_0", -1)
    xpb, xmb = shift(gb, "row_0", 1), shift(gb, "row_0", -1)
    x2a, x2b = shift(xpa, "row_0", 1), shift(xmb, "row_0", -1)
    gw = jnp.concatenate([own, w_block], axis=0)
    yp, ym = shift(gw, "col_0", 1), shift(gw, "col_0", -1)
    y2a, y2b = shift(yp[:ROWS], "col_0", 1), shift(ym[ROWS:], "col_0", -1)
    same_core = [ga, gb, xpa, xpb, xma, xmb, x2a, x2b]
    sibling = [shift(v, "row_2", 1) for v in same_core]
    blocks = same_core + sibling + [w_block, yp, ym, y2a, y2b]

    wide = jax.ShapeDtypeStruct((ROWS, D), F32)
    stat = jax.ShapeDtypeStruct((VIRT, D + 128), F32)
    queries, best, total, summed, part, own_part = pl.pallas_call(
        local_kernel,
        out_shape=[jax.ShapeDtypeStruct((ROWS, D), BF16), wide, wide, wide, stat, stat],
        in_specs=vmem(4),
        out_specs=vmem(6),
        compiler_params=pltpu.CompilerParams(vmem_limit_bytes=32 * 2**20),
        cost_estimate=cost(10_000_000_000, 4_000_000),
        name="local",
    )(node_states, virtual_states, gain, qkv_weight)

    part = reduce_virtual(part)
    virtual_out = pl.pallas_call(
        virtual_kernel,
        out_shape=jax.ShapeDtypeStruct((VIRT, D), BF16),
        in_specs=vmem(4),
        out_specs=pl.BlockSpec(memory_space=pltpu.VMEM),
        cost_estimate=cost(10_000_000, 400_000),
        name="virtual",
    )(part, own_part, virtual_states, out_weight)

    index = table_rows(neighbours)
    index = index.reshape(STEPS, BLOCK, DEG).transpose(0, 2, 1).reshape(ROWS * DEG)
    node_out = pl.pallas_call(
        lambda *refs: node_kernel(len(blocks), *refs),
        out_shape=jax.ShapeDtypeStruct((ROWS, D), BF16),
        in_specs=[pl.BlockSpec(memory_space=pltpu.SMEM)]
        + vmem(9)
        + [pl.BlockSpec(memory_space=pl.ANY)] * len(blocks),
        out_specs=pl.BlockSpec(memory_space=pltpu.VMEM),
        scratch_shapes=[
            pltpu.VMEM((TABLE * ROWS, D), BF16),
            pltpu.VMEM((2, TABLE * ROWS, 128), F32),
            pltpu.VMEM((2, ROWS * DEG, 128), F32),
            pltpu.SemaphoreType.DMA((TABLE,)),
        ],
        compiler_params=pltpu.CompilerParams(vmem_limit_bytes=60 * 2**20),
        cost_estimate=cost(30_000_000_000, 12_000_000),
        name="node",
    )(
        index,
        node_states,
        queries,
        best,
        total,
        summed,
        counts.reshape(ROWS, 1),
        gain,
        qkv_weight[:, D:],
        out_weight,
        *blocks,
    )
    return (node_out, virtual_out)


def solution(mesh):
    finer = Mesh(mesh.devices.reshape(4, 4, 2, 4, 2), AXES)
    in_specs = (P(AXES, None), P(AXES, None), P(AXES), P(), P(), P(), P())
    return jax.shard_map(
        shards, mesh=finer, in_specs=in_specs, out_specs=(P(AXES, None), P()), check_vma=False
    )
```
